32 devices in a mesh: tm: 8 (over z, y), rows: 4 (over x, core).
Axes of the slice: x: 2, y: 2, z: 4, core: 2. Of those that a mesh axis runs over, the one named last changes fastest.
Arguments:
- upstream: bfloat16 [32, 32, 128, 128], P('tm', 'rows'), may hold values from -6 to 6
- saved_first: bfloat16 [32, 32, 128, 128], P('tm', 'rows'), may hold values from -8 to 8
- saved_second: bfloat16 [32, 32, 128, 128], P('tm', 'rows'), may hold values from -8 to 8
- weight_first: bfloat16 [3456, 128], replicated, may hold values from -0.109375 to 0.109375
- weight_second: bfloat16 [3456, 128], replicated, may hold values from -0.109375 to 0.109375
Outputs:
- grad_input: bfloat16 [32, 32, 128, 128], P('tm', 'rows')
- wgrad_first: float32 [3456, 128], P('tm')
- wgrad_second: float32 [3456, 128], P('tm')
The draws below stay inside these ranges and needn't reach their ends.
All inputs are finite; a program needn't handle non-finite values.
Results may differ from the reference program's by a relative error of at most 0.005.
Values may be sent and summed in bfloat16 or wider, within the bound.
A program may use at most 64 MiB of HBM per device.

```python
import math
import jax
import jax.numpy as jnp
from jax import lax

CH = 128
COLS = 128
NF = 32
NR = 32


def draw_upstream(key, part):
    shape = (NF, NR, COLS, CH)
    offset = 4.0 / math.sqrt(NF * NR * COLS)
    values = jnp.clip(jax.random.normal(key, shape, jnp.float32), -5.9, 5.9)
    return jnp.clip(values + offset, -6.0, 6.0).astype(jnp.bfloat16)


def level_of(stream_key, extent, split, least, top_value):
    factor_of, own = 1.0, jax.random.fold_in(stream_key, 6)
    for position, parts in split:
        draws = jnp.exp(jax.random.uniform(jax.random.fold_in(own, position), (parts,), jnp.float32, least / len(split), top_value / len(split)))
        factor_of = factor_of * jnp.repeat(draws, extent[position] // parts).reshape([-1 if axis == position else 1 for axis in range(len(extent))])
    return factor_of


def centred(rng, shape, deviation, most, cuts=(), kind=jnp.bfloat16):
    array = deviation * jax.random.normal(rng, shape, jnp.float32)
    if cuts:
        array = array * level_of(rng, shape, cuts, -0.22, 0.18)
    return jnp.clip(array, -most, most).astype(kind)


def setup_inputs(seed: int = 0) -> dict:
    seeds = jax.random.split(jax.random.key(seed), 6)
    return {
        "upstream": draw_upstream(jax.random.fold_in(seeds[5], 71), 0),
        "saved_first": centred(seeds[1], (NF, NR, COLS, CH), 1.5, 8.0, ((0, 8), (1, 4))),
        "saved_second": centred(seeds[2], (NF, NR, COLS, CH), 1.5, 8.0, ((0, 8), (1, 4))),
        "weight_first": centred(seeds[3], (27 * CH, CH), (27 * CH) ** -0.5, 0.109375),
        "weight_second": centred(seeds[4], (27 * CH, CH), (27 * CH) ** -0.5, 0.109375),
    }


def silu_slope(value):
    sigma = jax.nn.sigmoid(value)
    return sigma * (1.0 + value * (1.0 - sigma))

def taps_frame(padded, frame, height, width):
    slab = lax.dynamic_slice_in_dim(padded, frame, 3, 0)
    pieces = []
    for shift_t in range(3):
        for shift_r in range(3):
            for shift_c in range(3):
                pieces.append(slab[2 - shift_t, 2 - shift_r:2 - shift_r + height, 2 - shift_c:2 - shift_c + width])
    return jnp.concatenate(pieces, axis=-1).reshape(height * width, -1)

def layer_back(grad_out, saved, weight):
    frames, height, width, chans = grad_out.shape
    padded = jnp.pad(grad_out, ((0, 2), (1, 1), (1, 1), (0, 0)))
    flipped = weight.reshape(27, chans, chans).transpose(0, 2, 1).reshape(27 * chans, chans)
    active = jax.nn.silu(saved.astype(jnp.float32)).astype(jnp.bfloat16)

    def one_frame(total, frame):
        columns = taps_frame(padded, frame, height, width)
        spread = jnp.dot(columns, flipped, preferred_element_type=jnp.float32)
        local_act = lax.dynamic_index_in_dim(active, frame, 0, keepdims=False).reshape(height * width, chans)
        total = total + jnp.dot(local_act.T, columns, preferred_element_type=jnp.float32)
        local_saved = lax.dynamic_index_in_dim(saved, frame, 0, keepdims=False).astype(jnp.float32)
        result = (spread.reshape(height, width, chans) * silu_slope(local_saved)).astype(jnp.bfloat16)
        return (total, result)
    start = jnp.zeros((chans, 27 * chans), jnp.float32)
    total, grads = lax.scan(one_frame, start, jnp.arange(frames, dtype=jnp.int32))
    wsum = total.reshape(chans, 27, chans).transpose(1, 0, 2).reshape(27 * chans, chans)
    return (grads, wsum)

def reference(upstream, saved_first, saved_second, weight_first, weight_second):
    grad_mid, wsum_second = layer_back(upstream, saved_second, weight_second)
    grad_input, wsum_first = layer_back(grad_mid, saved_first, weight_first)
    factor = 1.0 / math.sqrt(upstream.shape[0] * upstream.shape[1] * upstream.shape[2])
    return (grad_input, wsum_first * factor, wsum_second * factor)
```

```python
import functools
import math

import jax
import jax.numpy as jnp
from jax import lax
from jax.experimental import pallas as pl
from jax.experimental.pallas import tpu as pltpu
from jax.sharding import PartitionSpec as P

F32, BF16 = jnp.float32, jnp.bfloat16
VMEM_LIMIT = 60 * 1024 * 1024


def shifted(block, axis, step):
    count = lax.axis_size(axis)
    route = [(i - step, i) for i in range(count) if 0 <= i - step < count]
    return lax.ppermute(block, axis, route)


def halos(grad):
    height = grad.shape[1]
    above = shifted(grad[:, height - 1 :], "rows", 1)
    below = shifted(grad[:, :1], "rows", -1)
    later = shifted(grad[:2], "tm", -1)
    later_edges = shifted(jnp.concatenate([above[:2], below[:2]], axis=1), "tm", -1)
    return above, below, later, later_edges


def fill_row(cols, value, frame, row, height, width, chans):
    wide = value.astype(F32)
    place = lax.broadcasted_iota(jnp.int32, (width, chans), 0)
    after = jnp.where(place == width - 1, 0.0, pltpu.roll(wide, width - 1, 0)).astype(BF16)
    before = jnp.where(place == 0, 0.0, pltpu.roll(wide, 1, 0)).astype(BF16)
    for q in range(3):
        out_row = row - 1 + q
        if not 0 <= out_row < height:
            continue
        base = (frame * 9 + q * 3) * chans
        lines = pl.ds(out_row * width, width)
        cols[lines, pl.ds(base, chans)] = after
        cols[lines, pl.ds(base + chans, chans)] = value
        cols[lines, pl.ds(base + 2 * chans, chans)] = before


def fill(cols, grad_ref, above_ref, below_ref, later_ref, edges_ref):
    frames, height, width, chans = grad_ref.shape
    put = functools.partial(fill_row, cols, height=height, width=width, chans=chans)
    for frame in range(frames + 2):
        late = frame - frames
        if late < 0:
            first, last = above_ref[frame, 0], below_ref[frame, 0]
        else:
            first, last = edges_ref[late, 0], edges_ref[late, 1]
        put(first, frame, -1)
        put(last, frame, height)
        for row in range(height):
            put(grad_ref[frame, row] if late < 0 else later_ref[late, row], frame, row)


def spread_kernel(grad_ref, above_ref, below_ref, later_ref, edges_ref, saved_ref, weight_ref, out_ref, cols, kernels):
    frames, height, width, chans = grad_ref.shape
    span = 9 * chans
    for half in range(2):
        for j in range(4):
            p = 2 + half - j
            for tap in range(9):
                block = (
                    weight_ref[pl.ds((9 * p + tap) * chans, chans), :]
                    if 0 <= p < 3
                    else jnp.zeros((chans, chans), BF16)
                )
                kernels[pl.ds(half * chans, chans), pl.ds(j * span + tap * chans, chans)] = block
    fill(cols, grad_ref, above_ref, below_ref, later_ref, edges_ref)
    step_rows = math.gcd(4, height)
    lines = step_rows * width
    for pair in range(frames // 2):

        def chunk(index, carry, pair=pair):
            part = cols[pl.ds(pl.multiple_of(index * lines, lines), lines), pl.ds(pair * 2 * span, 4 * span)]
            spread = lax.dot_general(part, kernels[...], (((1,), (1,)), ((), ())), preferred_element_type=F32)
            for half in range(2):
                rows = pl.ds(index * step_rows, step_rows)
                value = saved_ref[2 * pair + half, rows].reshape(lines, chans).astype(F32)
                sigma = jax.nn.sigmoid(value)
                slope = sigma * (1.0 + value * (1.0 - sigma))
                result = spread[:, half * chans : (half + 1) * chans] * slope
                out_ref[2 * pair + half, rows] = result.astype(BF16).reshape(step_rows, width, chans)
            return carry

        lax.fori_loop(0, height // step_rows, chunk, 0)


def wsum_kernel(grad_ref, above_ref, below_ref, later_ref, edges_ref, saved_ref, out_ref, cols, active):
    frames, height, width, chans = grad_ref.shape
    span = 9 * chans
    fill(cols, grad_ref, above_ref, below_ref, later_ref, edges_ref)
    for frame in range(frames):
        for row in range(height):
            value = saved_ref[frame, row].astype(F32)
            act = value * jax.nn.sigmoid(value)
            active[pl.ds(frame * chans, chans), pl.ds(row * width, width)] = act.T.astype(BF16)
    out_ref[...] = jnp.zeros_like(out_ref)
    for frame in range(frames + 2):
        low, high = max(0, frame - 2), min(frames, frame + 1)
        acts = active[pl.ds(low * chans, (high - low) * chans), :]
        for q in range(3):
            part = cols[:, pl.ds(frame * span + q * 3 * chans, 3 * chans)]
            total = jnp.dot(acts, part, preferred_element_type=F32)
            for s in range(low, high):
                p = s + 2 - frame
                for k in range(3):
                    rows = pl.ds((9 * p + 3 * q + k) * chans, chans)
                    out_ref[rows, :] += total[(s - low) * chans : (s - low + 1) * chans, k * chans : (k + 1) * chans]


def vmem(count):
    return [pl.BlockSpec(memory_space=pltpu.VMEM)] * count


def spread_of(pieces, saved, weight):
    frames, height, width, chans = saved.shape
    flops = 2 * frames * height * width * 36 * chans * chans
    return pl.pallas_call(
        spread_kernel,
        out_shape=jax.ShapeDtypeStruct(saved.shape, BF16),
        in_specs=vmem(7),
        out_specs=pl.BlockSpec(memory_space=pltpu.VMEM),
        scratch_shapes=[
            pltpu.VMEM((height * width, (frames + 2) * 9 * chans), BF16),
            pltpu.VMEM((2 * chans, 36 * chans), BF16),
        ],
        compiler_params=pltpu.CompilerParams(vmem_limit_bytes=VMEM_LIMIT),
        cost_estimate=pl.CostEstimate(flops=flops, bytes_accessed=4 * saved.size, transcendentals=0),
        name="spread",
    )(*pieces, saved, weight)


def wsum_of(pieces, saved):
    frames, height, width, chans = saved.shape
    flops = 2 * frames * height * width * 27 * chans * chans
    return pl.pallas_call(
        wsum_kernel,
        out_shape=jax.ShapeDtypeStruct((27 * chans, chans), F32),
        in_specs=vmem(6),
        out_specs=pl.BlockSpec(memory_space=pltpu.VMEM),
        scratch_shapes=[
            pltpu.VMEM((height * width, (frames + 2) * 9 * chans), BF16),
            pltpu.VMEM((frames * chans, height * width), BF16),
        ],
        compiler_params=pltpu.CompilerParams(vmem_limit_bytes=VMEM_LIMIT),
        cost_estimate=pl.CostEstimate(flops=flops, bytes_accessed=4 * saved.size, transcendentals=0),
        name="wsum",
    )(*pieces, saved)


def reduced(wsum):
    depth, chans = wsum.shape
    slots, bands = lax.axis_size("tm"), lax.axis_size("rows")
    share = depth // slots
    if share % bands:
        return lax.psum_scatter(lax.psum(wsum, "rows"), "tm", scatter_dimension=0, tiled=True)
    parts = wsum.reshape(slots, bands, share // bands, chans)
    banded = lax.psum_scatter(parts, "rows", scatter_dimension=1, tiled=True)
    mine = lax.psum_scatter(banded, "tm", scatter_dimension=0, tiled=True)
    return lax.all_gather(mine.reshape(share // bands, chans), "rows", axis=0, tiled=True)


def body(upstream, saved_first, saved_second, weight_first, weight_second):
    pieces = (upstream, *halos(upstream))
    grad_mid = spread_of(pieces, saved_second, weight_second)
    pieces_mid = (grad_mid, *halos(grad_mid))
    wsum_second = wsum_of(pieces, saved_second)
    grad_input = spread_of(pieces_mid, saved_first, weight_first)
    wsum_first = wsum_of(pieces_mid, saved_first)
    frames, height, width, chans = upstream.shape
    factor = 1.0 / math.sqrt(frames * lax.axis_size("tm") * height * lax.axis_size("rows") * width)
    return (grad_input, reduced(wsum_first) * factor, reduced(wsum_second) * factor)


def solution(mesh):
    grid = P("tm", "rows", None, None)
    return jax.shard_map(
        body,
        mesh=mesh,
        in_specs=(grid, grid, grid, P(), P()),
        out_specs=(grid, P("tm", None), P("tm", None)),
        check_vma=False,
    )
```

```python
import functools
import math

import jax
import jax.numpy as jnp
from jax import lax
from jax.experimental import pallas as pl
from jax.experimental.pallas import tpu as pltpu
from jax.sharding import PartitionSpec as P

F32, BF16 = jnp.float32, jnp.bfloat16
VMEM_LIMIT = 60 * 1024 * 1024


def shifted(block, axis, step):
    count = lax.axis_size(axis)
    route = [(i - step, i) for i in range(count) if 0 <= i - step < count]
    return lax.ppermute(block, axis, route)


def halos(grad):
    height = grad.shape[1]
    above = shifted(grad[:, height - 1 :], "rows", 1)
    below = shifted(grad[:, :1], "rows", -1)
    later = shifted(grad[:2], "tm", -1)
    later_edges = shifted(jnp.concatenate([above[:2], below[:2]], axis=1), "tm", -1)
    return above, below, later, later_edges


def fill_row(cols, value, frame, row, height, width, chans):
    wide = value.astype(F32)
    place = lax.broadcasted_iota(jnp.int32, (width, chans), 0)
    after = jnp.where(place == width - 1, 0.0, pltpu.roll(wide, width - 1, 0)).astype(BF16)
    before = jnp.where(place == 0, 0.0, pltpu.roll(wide, 1, 0)).astype(BF16)
    for q in range(3):
        out_row = row - 1 + q
        if not 0 <= out_row < height:
            continue
        base = (frame * 9 + q * 3) * chans
        lines = pl.ds(out_row * width, width)
        cols[lines, pl.ds(base, chans)] = after
        cols[lines, pl.ds(base + chans, chans)] = value
        cols[lines, pl.ds(base + 2 * chans, chans)] = before


def fill(cols, grad_ref, above_ref, below_ref, later_ref, edges_ref):
    frames, height, width, chans = grad_ref.shape
    put = functools.partial(fill_row, cols, height=height, width=width, chans=chans)
    for frame in range(frames + 2):
        late = frame - frames
        if late < 0:
            first, last = above_ref[frame, 0], below_ref[frame, 0]
        else:
            first, last = edges_ref[late, 0], edges_ref[late, 1]
        put(first, frame, -1)
        put(last, frame, height)
        for row in range(height):
            put(grad_ref[frame, row] if late < 0 else later_ref[late, row], frame, row)


def spread_kernel(grad_ref, above_ref, below_ref, later_ref, edges_ref, saved_ref, weight_ref, out_ref, cols, kernels):
    frames, height, width, chans = grad_ref.shape
    span = 9 * chans
    for half in range(2):
        for j in range(4):
            p = 2 + half - j
            for tap in range(9):
                block = (
                    weight_ref[pl.ds((9 * p + tap) * chans, chans), :]
                    if 0 <= p < 3
                    else jnp.zeros((chans, chans), BF16)
                )
                kernels[pl.ds(half * chans, chans), pl.ds(j * span + tap * chans, chans)] = block
    fill(cols, grad_ref, above_ref, below_ref, later_ref, edges_ref)
    step_rows = math.gcd(4, height)
    lines = step_rows * width
    for pair in range(frames // 2):

        def chunk(index, carry, pair=pair):
            part = cols[pl.ds(pl.multiple_of(index * lines, lines), lines), pl.ds(pair * 2 * span, 4 * span)]
            spread = lax.dot_general(part, kernels[...], (((1,), (1,)), ((), ())), preferred_element_type=F32)
            for half in range(2):
                rows = pl.ds(index * step_rows, step_rows)
                value = saved_ref[2 * pair + half, rows].reshape(lines, chans).astype(F32)
                sigma = jax.nn.sigmoid(value)
                slope = sigma * (1.0 + value * (1.0 - sigma))
                result = spread[:, half * chans : (half + 1) * chans] * slope
                out_ref[2 * pair + half, rows] = result.astype(BF16).reshape(step_rows, width, chans)
            return carry

        lax.fori_loop(0, height // step_rows, chunk, 0)


def wsum_kernel(grad_ref, above_ref, below_ref, later_ref, edges_ref, saved_ref, out_ref, cols, active):
    frames, height, width, chans = grad_ref.shape
    span = 9 * chans
    fill(cols, grad_ref, above_ref, below_ref, later_ref, edges_ref)
    for frame in range(frames):
        for row in range(height):
            value = saved_ref[frame, row].astype(F32)
            act = value * jax.nn.sigmoid(value)
            active[pl.ds(frame * chans, chans), pl.ds(row * width, width)] = act.T.astype(BF16)
    out_ref[...] = jnp.zeros_like(out_ref)
    for frame in range(frames + 2):
        low, high = max(0, frame - 2), min(frames, frame + 1)
        acts = active[pl.ds(low * chans, (high - low) * chans), :]
        for q in range(3):
            part = cols[:, pl.ds(frame * span + q * 3 * chans, 3 * chans)]
            total = jnp.dot(acts, part, preferred_element_type=F32)
            for s in range(low, high):
                p = s + 2 - frame
                for k in range(3):
                    rows = pl.ds((9 * p + 3 * q + k) * chans, chans)
                    out_ref[rows, :] += total[(s - low) * chans : (s - low + 1) * chans, k * chans : (k + 1) * chans]


def vmem(count):
    return [pl.BlockSpec(memory_space=pltpu.VMEM)] * count


def spread_of(pieces, saved, weight):
    frames, height, width, chans = saved.shape
    flops = 2 * frames * height * width * 36 * chans * chans
    return pl.pallas_call(
        spread_kernel,
        out_shape=jax.ShapeDtypeStruct(saved.shape, BF16),
        in_specs=vmem(7),
        out_specs=pl.BlockSpec(memory_space=pltpu.VMEM),
        scratch_shapes=[
            pltpu.VMEM((height * width, (frames + 2) * 9 * chans), BF16),
            pltpu.VMEM((2 * chans, 36 * chans), BF16),
        ],
        compiler_params=pltpu.CompilerParams(vmem_limit_bytes=VMEM_LIMIT),
        cost_estimate=pl.CostEstimate(flops=flops, bytes_accessed=4 * saved.size, transcendentals=0),
        name="spread",
    )(*pieces, saved, weight)


def wsum_of(pieces, saved):
    frames, height, width, chans = saved.shape
    flops = 2 * frames * height * width * 27 * chans * chans
    return pl.pallas_call(
        wsum_kernel,
        out_shape=jax.ShapeDtypeStruct((27 * chans, chans), F32),
        in_specs=vmem(6),
        out_specs=pl.BlockSpec(memory_space=pltpu.VMEM),
        scratch_shapes=[
            pltpu.VMEM((height * width, (frames + 2) * 9 * chans), BF16),
            pltpu.VMEM((frames * chans, height * width), BF16),
        ],
        compiler_params=pltpu.CompilerParams(vmem_limit_bytes=VMEM_LIMIT),
        cost_estimate=pl.CostEstimate(flops=flops, bytes_accessed=4 * saved.size, transcendentals=0),
        name="wsum",
    )(*pieces, saved)


def exchanged_sum(parts, axis, dim):
    return jnp.sum(lax.all_to_all(parts, axis, split_axis=dim, concat_axis=dim, tiled=True), axis=dim)


def reduced(wsum_first, wsum_second, factor):
    depth, chans = wsum_first.shape
    slots, bands = lax.axis_size("tm"), lax.axis_size("rows")
    share = depth // slots
    if share % bands:
        first, second = lax.psum((wsum_first, wsum_second), "rows")
        both = jnp.stack([first.reshape(slots, share, chans), second.reshape(slots, share, chans)], axis=1)
        mine = exchanged_sum(both, "tm", 0) * factor
        return mine[0], mine[1]
    split = (slots, bands, share // bands, chans)
    second = lax.psum_scatter(wsum_second.reshape(split), "rows", scatter_dimension=1, tiled=False)
    first = exchanged_sum(wsum_first.reshape(split), "rows", 1)
    mine = exchanged_sum(jnp.stack([first, second], axis=1), "tm", 0) * factor
    whole = lax.all_gather(mine, "rows", axis=1, tiled=True)
    return whole[0], whole[1]


def body(upstream, saved_first, saved_second, weight_first, weight_second):
    pieces = (upstream, *halos(upstream))
    grad_mid = spread_of(pieces, saved_second, weight_second)
    pieces_mid = (grad_mid, *halos(grad_mid))
    wsum_second = wsum_of(pieces, saved_second)
    grad_input = spread_of(pieces_mid, saved_first, weight_first)
    wsum_first = wsum_of(pieces_mid, saved_first)
    frames, height, width, chans = upstream.shape
    factor = 1.0 / math.sqrt(frames * lax.axis_size("tm") * height * lax.axis_size("rows") * width)
    return (grad_input, *reduced(wsum_first, wsum_second, factor))


def solution(mesh):
    grid = P("tm", "rows", None, None)
    return jax.shard_map(
        body,
        mesh=mesh,
        in_specs=(grid, grid, grid, P(), P()),
        out_specs=(grid, P("tm", None), P("tm", None)),
        check_vma=False,
    )
```
